32 devices in a mesh: ops: 8 (over z, core), blk: 4 (over y, x).
Axes of the slice: x: 2, y: 2, z: 4, core: 2. Of those that a mesh axis runs over, the one named last changes fastest.
Arguments:
- psi: bfloat16 [2048, 1024], P('blk'), may hold values from -6 to 6
- left_blocks: bfloat16 [64, 16, 128, 128], P('ops', 'blk'), may hold values from -0.5 to 0.5
- right_ops: bfloat16 [64, 1024, 1024], P(('ops', 'blk')), may hold values from -0.046875 to 0.046875
- block_target: int32 [64, 16], P('ops'), may hold values from 0 to 15
- left_partner: int32 [64], P('ops'), may hold values from 0 to 63, as said below
- block_len: int32 [16], replicated, may hold values from 1 to 128, 1536 in all
Outputs:
- sigma: bfloat16 [2048, 1024], P('blk', 'ops')
The draws below stay inside these ranges and needn't reach their ends.
Inputs may be any that keep to these rules, and one draw needn't show every extreme that they name: left_partner is a permutation of 0 to 63 that maps each aligned group of 8 operators onto itself.
All inputs are finite; a program needn't handle non-finite values.
Results may differ from the reference program's by a relative error of at most 0.018.
Values may be sent and summed in bfloat16 or wider, within the bound.
A program may use at most 128 MiB of HBM per device.

```python
import math
import jax
import jax.numpy as jnp
import numpy as np
from jax import lax

BOND = 2048
BS = 128
RW = 1024
NB = 16
K = 64
OPS_GROUP = 8


def draw_left_partner(key, part):
    scores = jax.random.randint(key, (K,), 0, 65536, dtype=jnp.int32) * K + jnp.arange(K, dtype=jnp.int32)
    groups = K // OPS_GROUP
    order = jnp.argsort(scores.reshape(groups, OPS_GROUP), axis=1, stable=True).astype(jnp.int32)
    shifted = order + jnp.arange(groups, dtype=jnp.int32)[:, None] * OPS_GROUP
    return shifted.reshape(K).astype(jnp.int32)


def with_ends(values, stream_key, low, top_value):
    extent = values.shape
    place = [jax.random.randint(jax.random.fold_in(stream_key, axis), (), 0, extent[axis]) for axis in range(len(extent))]
    values = values.at[tuple(place)].set(low)
    longest = extent.index(max(extent))
    place[longest] = (place[longest] + 1) % extent[longest]
    return values.at[tuple(place)].set(top_value)


def with_spikes(array, rng, source, target, parts, factor):
    owner, partner = [(jnp.arange(array.shape[axis_at]) // (array.shape[axis_at] // parts)).reshape([-1 if axis == axis_at else 1 for axis in range(array.ndim)]) for axis_at in (source, target)]
    chosen = jax.random.permutation(rng, parts)[partner]
    strong = (owner == chosen) | (owner == (partner + parts // 2) % parts)
    return jnp.where(strong, factor * array, array)


def level_of(key, extent, split, smallest, top_value):
    factor_of = 1.0
    for position, parts in split:
        draws = jax.random.uniform(jax.random.fold_in(jax.random.fold_in(key, 6), position), (parts,), jnp.float32, smallest / len(split), top_value / len(split))
        factor_of = factor_of * jnp.repeat(jnp.exp(draws), extent[position] // parts).reshape((-1,) + (1,) * (len(extent) - 1 - position))
    return factor_of


def profile(count, total, reach, skew):
    weights = [(1 << 20) // math.isqrt(rank ** skew) + 1 for rank in range(2, count + 1)]
    surplus, holding = total - reach - (count - 1), [1] * (count - 1)
    while surplus > 0:
        candidates = [i for i in range(count - 1) if holding[i] < reach]
        mass, remaining = sum([weights[i] for i in candidates]), surplus
        for i in candidates:
            more = min(reach - holding[i], max(1, remaining * weights[i] // mass), surplus)
            holding[i] = holding[i] + more
            surplus = surplus - more
    return np.array([reach] + holding)


def uneven_parts(stream_key, amount, total, bound, skew):
    if amount == 2:
        one = jax.random.randint(stream_key, (), max(1, total - bound), min(bound, total - 1) + 1)
        return jnp.stack([one, total - one])
    lengths = jnp.asarray(profile(amount, total, bound, skew), jnp.int32)
    couples = (amount - 1) // 2
    source_of, taker = lengths[1:1 + 2 * couples:2], lengths[2:2 + 2 * couples:2]
    room = jnp.minimum(source_of - 1, bound - taker)
    moved = jax.random.randint(jax.random.fold_in(stream_key, 1), (couples,), 0, 1 << 20) % (room + 1)
    lengths = lengths.at[1:1 + 2 * couples:2].set(source_of - moved).at[2:2 + 2 * couples:2].set(taker + moved)
    return lengths[jax.random.permutation(jax.random.fold_in(stream_key, 2), amount)]


def noise(own_key, extent, scale, reach, shards=(), held_as=jnp.bfloat16):
    gain = level_of(own_key, extent, shards, -0.22, 0.18) if shards else 1.0
    values = jax.random.normal(own_key, extent, jnp.float32) * scale * gain
    return jnp.minimum(jnp.maximum(values, -reach), reach).astype(held_as)


def gaussian_with(own_key, shape, spread, limit, shards, heavy, kind=jnp.bfloat16):
    drawn = spread * jax.random.normal(own_key, shape, jnp.float32)
    if shards:
        drawn = drawn * level_of(own_key, shape, shards, -0.22, 0.18)
    return jnp.clip(with_spikes(drawn, jax.random.fold_in(own_key, 3), *heavy), -limit, limit).astype(kind)


def setup_inputs(seed: int = 0) -> dict:
    streams_of = jax.random.split(jax.random.key(seed), 7)
    psi = noise(streams_of[0], (BOND, RW), 1.0, 6.0, ((0, 4),))
    left_blocks = noise(streams_of[1], (K, NB, BS, BS), BS ** -0.5, 0.5, ((0, 8), (1, 4)))
    right_ops = gaussian_with(streams_of[2], (K, RW, RW), (RW * K) ** -0.5, 0.046875, ((0, 32),), (0, 2, 32, 2.75))
    block_target = with_ends(jax.random.randint(streams_of[3], (K, NB), 0, NB), jax.random.fold_in(streams_of[3], 1), 0, NB - 1).astype(jnp.int32)
    left_partner = draw_left_partner(jax.random.fold_in(streams_of[6], 71), 0)
    block_len = uneven_parts(streams_of[5], NB, 3 * BOND // 4, BS, 2).astype(jnp.int32)
    return dict(psi=psi, left_blocks=left_blocks, right_ops=right_ops, block_target=block_target, left_partner=left_partner, block_len=block_len)


def reference(psi, left_blocks, right_ops, block_target, left_partner, block_len):
    nblocks = BOND // BS
    row_index = jnp.arange(BS, dtype=jnp.int32)
    live_rows = row_index[None, :] < block_len[:, None]
    masked = psi.reshape(nblocks, BS, RW) * live_rows[:, :, None].astype(jnp.bfloat16)
    states = masked.reshape(BOND, RW).astype(jnp.float32)

    def absorb(totals, index):
        image = jnp.dot(states, right_ops[index].astype(jnp.float32), precision=lax.Precision.HIGHEST)
        image = lax.optimization_barrier(image.astype(jnp.bfloat16)).astype(jnp.float32)
        image = image.reshape(nblocks, BS, RW)
        owner = left_partner[index]
        mixed = jnp.einsum("qab,qbr->qar", left_blocks[owner].astype(jnp.float32), image, precision=lax.Precision.HIGHEST)
        totals = totals + jax.ops.segment_sum(mixed, block_target[owner], num_segments=nblocks)
        return totals, None

    start = jnp.zeros((nblocks, BS, RW), jnp.float32)
    totals = lax.scan(absorb, start, jnp.arange(K, dtype=jnp.int32))[0]
    result = totals * live_rows[:, :, None].astype(jnp.float32)
    return result.reshape(BOND, RW).astype(jnp.bfloat16)
```

```python
import functools

import jax
import jax.numpy as jnp
from jax import lax
from jax.experimental import pallas as pl
from jax.experimental.pallas import tpu as pltpu
from jax.sharding import PartitionSpec as P

MESH = pl.DeviceIdType.MESH
VMEM = pltpu.VMEM
DMA = pltpu.SemaphoreType.DMA


def across(c, d, n):
    out, bit = 0, 1
    while bit < n:
        have = (c // bit) % 2
        out = out + bit * (1 - have if d & bit else have)
        bit *= 2
    return out


def remote(src, dst, send, recv, to):
    return pltpu.make_async_remote_copy(
        src_ref=src, dst_ref=dst, send_sem=send, recv_sem=recv, device_id=to, device_id_type=MESH
    )


def greet(targets):
    barrier = pltpu.get_barrier_semaphore()
    for to in targets:
        pl.semaphore_signal(barrier, inc=1, device_id=to, device_id_type=MESH)
    pl.semaphore_wait(barrier, len(targets))


def places(n_ops, n_blk):
    g, c = lax.axis_index("ops"), lax.axis_index("blk")
    chips = n_ops // 2
    z, core = g // 2, g % 2
    peers = [across(c, d, n_blk) for d in range(n_blk)]
    up = [((z + e) % chips) * 2 + core for e in range(chips)]
    down = [((z + chips - e) % chips) * 2 + core for e in range(chips)]
    partner = z * 2 + (1 - core)
    return g, c, z, core, peers, up, down, partner


def gather_kernel(
    n_ops, n_blk, psi_ref, left_ref, pair_ref, psi_out, left_out, stage,
    send_a, recv_a, send_l, recv_l, send_b, recv_b, send_p, recv_p,
):
    g, c, z, core, peers, up, down, partner = places(n_ops, n_blk)
    chips = n_ops // 2
    piece = psi_ref.shape[0] // n_ops
    group = left_ref.shape[0]
    local_ops = group // n_blk
    rows = pl.ds(pl.multiple_of(g * piece, piece), piece)

    greet(
        [(g, peers[d]) for d in range(1, n_blk)]
        + [(up[e], c) for e in range(1, chips)]
        + [(partner, c)]
    )
    first = [
        remote(psi_ref.at[rows], psi_out.at[c, rows], send_a.at[d], recv_a.at[d], (g, peers[d]))
        for d in range(n_blk)
    ]
    order = list(range(n_blk - 1, 0, -1))
    for d in order:
        first[d].start()
    for j in range(group):
        stage[j] = left_ref[pair_ref[j]]
    lefts = [
        remote(
            stage.at[pl.ds(peers[d] * local_ops, local_ops)],
            left_out.at[c], send_l.at[d], recv_l.at[d], (g, peers[d]),
        )
        for d in range(n_blk)
    ]
    for d in order:
        lefts[d].start()
    psi_out[c] = psi_ref[...]
    left_out[c] = stage[pl.ds(c * local_ops, local_ops)]

    sent = []
    for d in order:
        first[d].wait_recv()
        here = psi_out.at[peers[d], rows]
        for e in range(1, chips):
            copy = remote(here, here, send_b.at[d, e], recv_b.at[d, e], (up[e], c))
            copy.start()
            sent.append(copy)
        copy = remote(here, here, send_p.at[d, 0], recv_p.at[d, 0], (partner, c))
        copy.start()
        sent.append(copy)
    for d in order:
        for e in range(1, chips):
            at = pl.ds(pl.multiple_of(down[e] * piece, piece), piece)
            here = psi_out.at[peers[d], at]
            remote(here, here, send_b.at[d, e], recv_b.at[d, e], (up[e], c)).wait_recv()
            copy = remote(here, here, send_p.at[d, e], recv_p.at[d, e], (partner, c))
            copy.start()
            sent.append(copy)
    for d in order:
        for e in range(chips):
            other = down[e] - core + (1 - core)
            at = pl.ds(pl.multiple_of(other * piece, piece), piece)
            here = psi_out.at[peers[d], at]
            remote(here, here, send_p.at[d, e], recv_p.at[d, e], (partner, c)).wait_recv()
        lefts[d].wait_recv()
    for copy in sent:
        copy.wait_send()
    for d in order:
        first[d].wait_send()
        lefts[d].wait_send()


def mix_kernel(target_ref, len_ref, psi_ref, left_ref, out_ref, total):
    blocks, block_rows, columns = psi_ref.shape
    local_ops = total.shape[0]
    per = left_ref.shape[2]
    total[...] = jnp.zeros_like(total)
    lane = lax.broadcasted_iota(jnp.int32, (1, block_rows), 1)

    def one(q, carry):
        left = left_ref[q // per, :, q % per].reshape(local_ops * block_rows, block_rows)
        left = jnp.where(lane < len_ref[q], left, jnp.zeros_like(left))
        for half in range(columns // 512):
            cols = pl.ds(half * 512, 512)
            mixed = jnp.dot(left, psi_ref[q, :, cols], preferred_element_type=jnp.float32)
            for r in range(local_ops):
                t = target_ref[r, q]
                total[r, t, :, cols] += mixed[r * block_rows : (r + 1) * block_rows]
        return carry

    lax.fori_loop(0, blocks, one, 0)

    def out(t, carry):
        for r in range(local_ops):
            out_ref[r, t] = total[r, t].astype(out_ref.dtype)
        return carry

    lax.fori_loop(0, blocks, out, 0)


def reduce_kernel(
    n_ops, n_blk, y_hbm, r_hbm, out_ref,
    y_v, r_v, part, recv1, send2, recv2, send3, recv3,
    y_sem, r_sem, send_1, recv_1, send_2, recv_2, send_3, recv_3,
):
    g, c, z, core, peers, up, down, partner = places(n_ops, n_blk)
    chips = n_ops // 2
    local_ops = r_v.shape[0]
    rows = y_v.shape[2]
    wide = 2 * out_ref.shape[1]
    thin = out_ref.shape[1]
    order = list(range(n_blk - 1, -1, -1))

    def load(d):
        at = pl.ds(pl.multiple_of(peers[d] * rows, rows), rows)
        return pltpu.make_async_copy(y_hbm.at[:, at], y_v.at[d], y_sem.at[d])

    weights = pltpu.make_async_copy(r_hbm, r_v, r_sem)
    load(order[0]).start()
    weights.start()
    for d in order[1:]:
        load(d).start()
    greet(
        [(g, peers[d]) for d in range(1, n_blk)]
        + [(up[e], c) for e in range(1, chips)]
        + [(partner, c)]
    )
    weights.wait()

    def compute(d):
        load(d).wait()

        def tile(j, carry):
            cols = pl.ds(pl.multiple_of(j * wide, wide), wide)
            acc = jnp.dot(y_v[d, 0], r_v[0, :, cols], preferred_element_type=jnp.float32)
            for r in range(1, local_ops):
                acc += jnp.dot(y_v[d, r], r_v[r, :, cols], preferred_element_type=jnp.float32)
            acc = acc.astype(jnp.bfloat16)
            part[d, 0, j] = acc[:, :thin]
            part[d, 1, j] = acc[:, thin:]
            return carry

        lax.fori_loop(0, chips, tile, 0)

    swaps = [
        remote(part.at[d, 1 - core], recv1.at[d], send_1.at[d], recv_1.at[d], (partner, c))
        for d in range(n_blk)
    ]
    outs = [
        remote(send2.at[d], recv2.at[d], send_2.at[d], recv_2.at[d], (g, peers[d]))
        for d in range(n_blk)
    ]

    def join(d):
        swaps[d].wait_recv()

        def add(j, carry):
            send2[d, j] = (
                part[d, core, j].astype(jnp.float32) + recv1[d, j].astype(jnp.float32)
            ).astype(jnp.bfloat16)
            return carry

        lax.fori_loop(0, chips, add, 0)
        if d:
            outs[d].start()

    before = None
    for d in order:
        compute(d)
        swaps[d].start()
        if before is not None:
            join(before)
        before = d
    join(before)
    for d in order[:-1]:
        outs[d].wait_recv()

    def gathered(j):
        acc = send2[0, j].astype(jnp.float32)
        for d in range(1, n_blk):
            acc += recv2[d, j].astype(jnp.float32)
        return acc

    lasts = [
        remote(send3.at[e], recv3.at[e], send_3.at[e], recv_3.at[e], (up[e], c))
        for e in range(chips)
    ]
    for e in range(1, chips):
        send3[e] = gathered((z + e) % chips).astype(jnp.bfloat16)
        lasts[e].start()
    acc = gathered(z)
    for e in range(1, chips):
        lasts[e].wait_recv()
        acc += recv3[e].astype(jnp.float32)
    out_ref[...] = acc.astype(out_ref.dtype)
    for d in range(n_blk):
        swaps[d].wait_send()
        if d:
            outs[d].wait_send()
    for e in range(1, chips):
        lasts[e].wait_send()


def local(n_ops, n_blk, psi, left_blocks, right_ops, block_target, left_partner, block_len):
    group, local_blocks, block_rows, _ = left_blocks.shape
    my_rows, columns = psi.shape
    local_ops = right_ops.shape[0]
    blocks = block_target.shape[1]
    chips = n_ops // 2
    thin = columns // n_ops
    bf16 = jnp.bfloat16
    in_vmem = pl.BlockSpec(memory_space=pltpu.VMEM)
    in_smem = pl.BlockSpec(memory_space=pltpu.SMEM)
    in_hbm = pl.BlockSpec(memory_space=pl.ANY)

    pair = left_partner - lax.axis_index("ops") * group
    psi_all, left_all = pl.pallas_call(
        functools.partial(gather_kernel, n_ops, n_blk),
        out_shape=(
            jax.ShapeDtypeStruct((n_blk, my_rows, columns), bf16),
            jax.ShapeDtypeStruct((n_blk, local_ops, local_blocks, block_rows, block_rows), bf16),
        ),
        in_specs=[in_vmem, in_vmem, in_smem],
        out_specs=(in_vmem, in_vmem),
        scratch_shapes=[
            VMEM(left_blocks.shape, bf16),
            DMA((n_blk,)), DMA((n_blk,)), DMA((n_blk,)), DMA((n_blk,)),
            DMA((n_blk, chips)), DMA((n_blk, chips)), DMA((n_blk, chips)), DMA((n_blk, chips)),
        ],
        compiler_params=pltpu.CompilerParams(collective_id=0, has_side_effects=True),
        name="gather",
    )(psi, left_blocks, pair)

    c = lax.axis_index("blk")
    mine = lax.dynamic_slice_in_dim(pair, c * local_ops, local_ops, 0)
    targets = block_target[mine]
    mixed = pl.pallas_call(
        mix_kernel,
        out_shape=jax.ShapeDtypeStruct((local_ops, blocks, block_rows, columns), bf16),
        in_specs=[in_smem, in_smem, in_vmem, in_vmem],
        out_specs=in_vmem,
        scratch_shapes=[VMEM((local_ops, blocks, block_rows, columns), jnp.float32)],
        compiler_params=pltpu.CompilerParams(vmem_limit_bytes=63 * 2**20),
        name="mix",
    )(targets, block_len, psi_all.reshape(blocks, block_rows, columns), left_all)

    sums = pl.pallas_call(
        functools.partial(reduce_kernel, n_ops, n_blk),
        out_shape=jax.ShapeDtypeStruct((my_rows, thin), bf16),
        in_specs=[in_hbm, in_hbm],
        out_specs=in_vmem,
        scratch_shapes=[
            VMEM((n_blk, local_ops, my_rows, columns), bf16),
            VMEM(right_ops.shape, bf16),
            VMEM((n_blk, 2, chips, my_rows, thin), bf16),
            VMEM((n_blk, chips, my_rows, thin), bf16),
            VMEM((n_blk, chips, my_rows, thin), bf16),
            VMEM((n_blk, chips, my_rows, thin), bf16),
            VMEM((chips, my_rows, thin), bf16),
            VMEM((chips, my_rows, thin), bf16),
            DMA((n_blk,)), DMA, DMA((n_blk,)), DMA((n_blk,)), DMA((n_blk,)), DMA((n_blk,)),
            DMA((chips,)), DMA((chips,)),
        ],
        compiler_params=pltpu.CompilerParams(
            collective_id=1, has_side_effects=True, vmem_limit_bytes=63 * 2**20
        ),
        name="reduce",
    )(mixed.reshape(local_ops, blocks * block_rows, columns), right_ops)

    lens = lax.dynamic_slice_in_dim(block_len, c * local_blocks, local_blocks, 0)
    live = jnp.arange(block_rows, dtype=jnp.int32)[None, :] < lens[:, None]
    shaped = sums.reshape(local_blocks, block_rows, thin)
    return jnp.where(live[:, :, None], shaped, jnp.zeros_like(shaped)).reshape(my_rows, thin)


def solution(mesh):
    return jax.shard_map(
        functools.partial(local, mesh.shape["ops"], mesh.shape["blk"]),
        mesh=mesh,
        in_specs=(
            P("blk", None),
            P("ops", "blk", None, None),
            P(("ops", "blk"), None, None),
            P("ops", None),
            P("ops"),
            P(),
        ),
        out_specs=P("blk", "ops"),
        check_vma=False,
    )
```

```python
import functools

import jax
import jax.numpy as jnp
from jax import lax
from jax.experimental import pallas as pl
from jax.experimental.pallas import tpu as pltpu
from jax.sharding import PartitionSpec as P

MESH = pl.DeviceIdType.MESH
VMEM = pltpu.VMEM
DMA = pltpu.SemaphoreType.DMA


def across(c, d, n):
    out, bit = 0, 1
    while bit < n:
        have = (c // bit) % 2
        out = out + bit * (1 - have if d & bit else have)
        bit *= 2
    return out


def remote(src, dst, send, recv, to):
    return pltpu.make_async_remote_copy(
        src_ref=src, dst_ref=dst, send_sem=send, recv_sem=recv, device_id=to, device_id_type=MESH
    )


def greet(targets):
    barrier = pltpu.get_barrier_semaphore()
    for to in targets:
        pl.semaphore_signal(barrier, inc=1, device_id=to, device_id_type=MESH)
    pl.semaphore_wait(barrier, len(targets))


def places(n_ops, n_blk):
    g, c = lax.axis_index("ops"), lax.axis_index("blk")
    chips = n_ops // 2
    z, core = g // 2, g % 2
    peers = [across(c, d, n_blk) for d in range(n_blk)]
    up = [((z + e) % chips) * 2 + core for e in range(chips)]
    down = [((z + chips - e) % chips) * 2 + core for e in range(chips)]
    partner = z * 2 + (1 - core)
    return g, c, z, core, peers, up, down, partner


def shares(my_rows, n_ops):
    piece = max(my_rows * 3 // 4 // n_ops // 16, 1) * 16
    return piece, (my_rows - piece * n_ops) // 2


def gather_kernel(
    n_ops, n_blk, psi_ref, left_ref, pair_ref, psi_out, left_out, stage,
    send_a, recv_a, send_l, recv_l, send_c, recv_c, send_z, recv_z, send_p, recv_p,
):
    g, c, z, core, peers, up, down, partner = places(n_ops, n_blk)
    chips = n_ops // 2
    piece, straight = shares(psi_ref.shape[0], n_ops)
    group = left_ref.shape[0]
    local_ops = group // n_blk

    def rows_of(chip, which):
        return pl.ds(pl.multiple_of((chip * 2 + which) * piece, piece), piece)

    def straight_of(which):
        return pl.ds(pl.multiple_of(piece * n_ops + which * straight, 16), straight)

    greet(
        [(g, peers[d]) for d in range(1, n_blk)]
        + [(up[1], c), (down[1], c), (partner, c)]
    )
    order = list(range(1, n_blk))
    mine = rows_of(z, core)
    first = {
        d: remote(psi_ref.at[mine], psi_out.at[c, mine], send_a.at[d], recv_a.at[d], (g, peers[d]))
        for d in order
    }
    for d in order:
        first[d].start()
    for j in range(group):
        stage[j] = left_ref[lax.rem(pair_ref[j], group)]
    lefts = {
        d: remote(
            stage.at[pl.ds(peers[d] * local_ops, local_ops)],
            left_out.at[c], send_l.at[d], recv_l.at[d], (g, peers[d]),
        )
        for d in order
    }
    at = straight_of(core) if straight else None
    plain = {
        d: remote(psi_ref.at[at], psi_out.at[c, at], send_c.at[d], recv_c.at[d], (g, peers[d]))
        for d in order if straight
    }
    for d in order:
        if straight:
            plain[d].start()
    for d in order:
        lefts[d].start()
    psi_out[c] = psi_ref[...]
    left_out[c] = stage[pl.ds(c * local_ops, local_ops)]

    def hop(d, h, way, source):
        here = psi_out.at[peers[d], rows_of(source, core)]
        to = (g + 2, c) if way == 0 else (g - 2, c)
        return remote(here, here, send_z.at[way, d, h], recv_z.at[way, d, h], to)

    def share(d, h, way, source, which):
        here = psi_out.at[peers[d], rows_of(source, which)]
        return remote(here, here, send_p.at[way, d, h], recv_p.at[way, d, h], (partner, c))

    def can_send(h, way):
        if way == 0:
            return jnp.logical_and(z >= h, z < chips - 1)
        return jnp.logical_and(z < chips - h, z > 0)

    def has(h, way):
        return z >= h if way == 0 else z < chips - h

    def source_of(h, way):
        return z - h if way == 0 else z + h

    for h in range(chips):
        for d in order:
            if h == 0:
                first[d].wait_recv()
                share(d, 0, 0, z, core).start()
            for way in range(2):
                source = source_of(h, way)
                if h:
                    @pl.when(has(h, way))
                    def _(d=d, h=h, way=way, source=source):
                        hop(d, h - 1, way, source).wait_recv()
                        share(d, h, way, source, core).start()
                if h < chips - 1:
                    @pl.when(can_send(h, way))
                    def _(d=d, h=h, way=way, source=source):
                        hop(d, h, way, source).start()
    for d in order if straight else []:
        plain[d].wait_recv()
        here = psi_out.at[peers[d], at]
        remote(here, here, send_c.at[d + n_blk], recv_c.at[d + n_blk], (partner, c)).start()
    for d in order:
        if straight:
            here = psi_out.at[peers[d], straight_of(1 - core)]
            remote(here, here, send_c.at[d + n_blk], recv_c.at[d + n_blk], (partner, c)).wait()
            plain[d].wait_send()
        lefts[d].wait()
        first[d].wait_send()
        share(d, 0, 0, z, 1 - core).wait()
        for way in range(2):
            for h in range(chips):
                source = source_of(h, way)
                if h:
                    @pl.when(has(h, way))
                    def _(d=d, h=h, way=way, source=source):
                        share(d, h, way, source, 1 - core).wait()
                if h < chips - 1:
                    @pl.when(can_send(h, way))
                    def _(d=d, h=h, way=way, source=source):
                        hop(d, h, way, source).wait_send()


def mix_kernel(target_ref, pair_ref, len_ref, psi_ref, left_ref, out_ref, total):
    blocks, block_rows, columns = psi_ref.shape
    local_ops = total.shape[0]
    per = left_ref.shape[2]
    group = target_ref.shape[0]
    c = lax.axis_index("blk")
    total[...] = jnp.zeros_like(total)
    lane = lax.broadcasted_iota(jnp.int32, (1, block_rows), 1)
    row = lax.broadcasted_iota(jnp.int32, (block_rows, 1), 0)
    owners = [lax.rem(pair_ref[c * local_ops + r], group) for r in range(local_ops)]

    def one(q, carry):
        left = left_ref[q // per, :, q % per].reshape(local_ops * block_rows, block_rows)
        left = jnp.where(lane < len_ref[q], left, jnp.zeros_like(left))
        mixed = jnp.dot(left, psi_ref[q], preferred_element_type=jnp.float32)
        for r in range(local_ops):
            total[r, target_ref[owners[r], q]] += mixed[r * block_rows : (r + 1) * block_rows]
        return carry

    lax.fori_loop(0, blocks, one, 0, unroll=4)

    def out(t, carry):
        for r in range(local_ops):
            kept = total[r, t]
            kept = jnp.where(row < len_ref[t], kept, jnp.zeros_like(kept))
            out_ref[r, t] = kept.astype(out_ref.dtype)
        return carry

    lax.fori_loop(0, blocks, out, 0)


def reduce_kernel(
    n_ops, n_blk, y_hbm, r_hbm, out_ref,
    y_v, r_v, part, recv1, send2, recv2, send3, recv3,
    y_sem, r_sem, send_1, recv_1, send_2, recv_2, send_3, recv_3,
):
    g, c, z, core, peers, up, down, partner = places(n_ops, n_blk)
    chips = n_ops // 2
    local_ops = r_hbm.shape[0]
    rows = y_v.shape[2]
    thin = out_ref.shape[1]
    wide = 2 * thin
    order = list(range(n_blk - 1, -1, -1))

    def load(d):
        at = pl.ds(pl.multiple_of(peers[d] * rows, rows), rows)
        return pltpu.make_async_copy(y_hbm.at[:, at], y_v.at[d], y_sem.at[d])

    def weights(k):
        j = (z + 1 + k) % chips
        cols = pl.ds(pl.multiple_of(j * wide, wide), wide)
        return pltpu.make_async_copy(r_hbm.at[:, :, cols], r_v.at[k], r_sem.at[k])

    weights(0).start()
    for d in order:
        load(d).start()
    for k in range(1, chips):
        weights(k).start()
    greet(
        [(g, peers[d]) for d in range(1, n_blk)]
        + [(up[e], c) for e in range(1, chips)]
        + [(partner, c)]
    )

    def product(k, d):
        acc = jnp.dot(y_v[d, 0], r_v[k, 0], preferred_element_type=jnp.float32)
        for r in range(1, local_ops):
            acc += jnp.dot(y_v[d, r], r_v[k, r], preferred_element_type=jnp.float32)
        acc = acc.astype(jnp.bfloat16)
        part[k, 0, d] = acc[:, :thin]
        part[k, 1, d] = acc[:, thin:]

    def swap(k):
        return remote(
            part.at[k, 1 - core], recv1.at[k], send_1.at[k], recv_1.at[k], (partner, c)
        )

    def spread(k, d):
        return remote(
            send2.at[k, d], recv2.at[k, d], send_2.at[k, d], recv_2.at[k, d], (g, peers[d])
        )

    def last(k):
        return remote(
            send3.at[k], recv3.at[k], send_3.at[k], recv_3.at[k], (up[k + 1], c)
        )

    def compute(k):
        weights(k).wait()
        if k == 0:
            for d in order:
                load(d).wait()
                product(k, d)
        else:
            lax.fori_loop(0, n_blk, lambda d, carry: (product(k, d), carry)[1], 0)
        swap(k).start()

    def join(k):
        swap(k).wait_recv()
        for d in order:
            send2[k, d] = (
                part[k, core, d].astype(jnp.float32) + recv1[k, d].astype(jnp.float32)
            ).astype(jnp.bfloat16)
            if d:
                spread(k, d).start()

    def finish(k):
        acc = send2[k, 0].astype(jnp.float32)
        for d in range(1, n_blk):
            spread(k, d).wait_recv()
            acc += recv2[k, d].astype(jnp.float32)
        if k < chips - 1:
            send3[k] = acc.astype(jnp.bfloat16)
            last(k).start()
            return
        for e in range(chips - 1):
            last(e).wait_recv()
            acc += recv3[e].astype(jnp.float32)
        out_ref[...] = acc.astype(out_ref.dtype)

    compute(0)
    for k in range(1, chips):
        compute(k)
        join(k - 1)
        if k > 2:
            finish(k - 3)
    join(chips - 1)
    for k in range(max(chips - 3, 0), chips):
        finish(k)
    for k in range(chips):
        swap(k).wait_send()
        for d in range(1, n_blk):
            spread(k, d).wait_send()
        if k < chips - 1:
            last(k).wait_send()


def local(n_ops, n_blk, psi, left_blocks, right_ops, block_target, left_partner, block_len):
    group, local_blocks, block_rows, _ = left_blocks.shape
    my_rows, columns = psi.shape
    local_ops = right_ops.shape[0]
    blocks = block_target.shape[1]
    chips = n_ops // 2
    thin = columns // n_ops
    bf16 = jnp.bfloat16
    in_vmem = pl.BlockSpec(memory_space=pltpu.VMEM)
    in_smem = pl.BlockSpec(memory_space=pltpu.SMEM)
    in_hbm = pl.BlockSpec(memory_space=pl.ANY)

    psi_all, left_all = pl.pallas_call(
        functools.partial(gather_kernel, n_ops, n_blk),
        out_shape=(
            jax.ShapeDtypeStruct((n_blk, my_rows, columns), bf16),
            jax.ShapeDtypeStruct((n_blk, local_ops, local_blocks, block_rows, block_rows), bf16),
        ),
        in_specs=[in_vmem, in_vmem, in_smem],
        out_specs=(in_vmem, in_vmem),
        scratch_shapes=[
            VMEM(left_blocks.shape, bf16),
            DMA((n_blk,)), DMA((n_blk,)), DMA((n_blk,)), DMA((n_blk,)),
            DMA((2 * n_blk,)), DMA((2 * n_blk,)),
            DMA((2, n_blk, chips)), DMA((2, n_blk, chips)),
            DMA((2, n_blk, chips)), DMA((2, n_blk, chips)),
        ],
        compiler_params=pltpu.CompilerParams(collective_id=0, has_side_effects=True),
        name="gather",
    )(psi, left_blocks, left_partner)

    step = min(columns, 256)
    mixed = pl.pallas_call(
        mix_kernel,
        grid=(columns // step,),
        out_shape=jax.ShapeDtypeStruct((local_ops, blocks, block_rows, columns), bf16),
        in_specs=[
            in_smem, in_smem, in_smem,
            pl.BlockSpec((blocks, block_rows, step), lambda i: (0, 0, i)),
            pl.BlockSpec(left_all.shape, lambda i: (0,) * 5),
        ],
        out_specs=pl.BlockSpec((local_ops, blocks, block_rows, step), lambda i: (0, 0, 0, i)),
        scratch_shapes=[VMEM((local_ops, blocks, block_rows, step), jnp.float32)],
        compiler_params=pltpu.CompilerParams(vmem_limit_bytes=63 * 2**20),
        name="mix",
    )(
        block_target, left_partner, block_len,
        psi_all.reshape(blocks, block_rows, columns), left_all,
    )

    return pl.pallas_call(
        functools.partial(reduce_kernel, n_ops, n_blk),
        out_shape=jax.ShapeDtypeStruct((my_rows, thin), bf16),
        in_specs=[in_hbm, in_hbm],
        out_specs=in_vmem,
        scratch_shapes=[
            VMEM((n_blk, local_ops, my_rows, columns), bf16),
            VMEM((chips, local_ops, columns, 2 * thin), bf16),
            VMEM((chips, 2, n_blk, my_rows, thin), bf16),
            VMEM((chips, n_blk, my_rows, thin), bf16),
            VMEM((chips, n_blk, my_rows, thin), bf16),
            VMEM((chips, n_blk, my_rows, thin), bf16),
            VMEM((chips, my_rows, thin), bf16),
            VMEM((chips, my_rows, thin), bf16),
            DMA((n_blk,)), DMA((chips,)), DMA((chips,)), DMA((chips,)),
            DMA((chips, n_blk)), DMA((chips, n_blk)), DMA((chips,)), DMA((chips,)),
        ],
        compiler_params=pltpu.CompilerParams(
            collective_id=1, has_side_effects=True, vmem_limit_bytes=63 * 2**20
        ),
        name="reduce",
    )(mixed.reshape(local_ops, blocks * block_rows, columns), right_ops)


def solution(mesh):
    return jax.shard_map(
        functools.partial(local, mesh.shape["ops"], mesh.shape["blk"]),
        mesh=mesh,
        in_specs=(
            P("blk", None),
            P("ops", "blk", None, None),
            P(("ops", "blk"), None, None),
            P("ops", None),
            P("ops"),
            P(),
        ),
        out_specs=P("blk", "ops"),
        check_vma=False,
    )
```
